8 devices in a mesh: rep: 2 (over y, z), dp: 4 (over x, core).
Axes of the slice: x: 2, y: 2, z: 1, core: 2. Of those that a mesh axis runs over, the one named last changes fastest.
Arguments:
- x: bfloat16 [8, 2048, 1536], P(('rep', 'dp')), parts along dimension 0
- dy: bfloat16 [8, 2048, 1536], P(('rep', 'dp')), parts along dimension 0
- w_gate: bfloat16 [2, 1536, 4224], replicated
- w_up: bfloat16 [2, 1536, 4224], replicated
- w_down: bfloat16 [2, 4224, 1536], replicated
- m_w_gate: float32 [2, 1536, 4224], P(None, 'dp')
- m_w_up: float32 [2, 1536, 4224], P(None, 'dp')
- m_w_down: float32 [2, 4224, 1536], P(None, 'dp')
- v_w_gate: float32 [2, 1536, 4224], P(None, 'dp')
- v_w_up: float32 [2, 1536, 4224], P(None, 'dp')
- v_w_down: float32 [2, 4224, 1536], P(None, 'dp')
Outputs:
- output 1: bfloat16 [4, 1536, 4224], P('rep'), parts along dimension 0
- output 2: bfloat16 [4, 1536, 4224], P('rep'), parts along dimension 0
- output 3: bfloat16 [4, 4224, 1536], P('rep'), parts along dimension 0
- output 4: float32 [4, 1536, 4224], P('rep', 'dp'), parts along dimension 0
- output 5: float32 [4, 1536, 4224], P('rep', 'dp'), parts along dimension 0
- output 6: float32 [4, 4224, 1536], P('rep', 'dp'), parts along dimension 0
- output 7: float32 [4, 1536, 4224], P('rep', 'dp'), parts along dimension 0
- output 8: float32 [4, 1536, 4224], P('rep', 'dp'), parts along dimension 0
- output 9: float32 [4, 4224, 1536], P('rep', 'dp'), parts along dimension 0
There are 2 independent parts. The reference program is written for one: setup_inputs(seed, part) draws one part's arguments, and reference() takes and returns one part's arrays. A program takes and returns all parts, laid end to end along the dimension named above; an argument that names none is the same for every part.
All inputs are finite; a program needn't handle non-finite values.
Results may differ from the reference program's by a relative error of at most 0.02.
Values are sent between devices in bfloat16 or wider.
A program may use at most 2 GiB of HBM per device.

```python
import jax
import jax.numpy as jnp
from jax import lax

SEQUENCES = 4
TOKENS = 2048
D = 1536
FF = 4224
LAYERS = 2
NAMES = ("w_gate", "w_up", "w_down")
SHAPES = {"w_gate": (LAYERS, D, FF), "w_up": (LAYERS, D, FF), "w_down": (LAYERS, FF, D)}


def bump(key, n, height):
    away = (jnp.arange(n, dtype=jnp.int32) - jax.random.randint(key, (), 0, n, jnp.int32)) % n
    return jnp.where(away < n // 8, height, 1.0)


def together(key, own, strength):
    shared = jax.random.normal(key, own.shape[1:], jnp.float32)
    return (own + strength * shared) * lax.rsqrt(1 + strength * strength)


def setup_inputs(seed: int = 0, part: int = 0) -> dict:
    kx, kdy, ka, kb, kz, kf, kh, kl, *keys = jax.random.split(jax.random.key(seed), 8 + 3 * len(NAMES))
    kx, kdy, ka, kb = (jax.random.fold_in(k, part) for k in (kx, kdy, ka, kb))
    kw, km, kv = (keys[i::3] for i in range(3))
    shape = (SEQUENCES, TOKENS, D)
    much_x, much_dy = jax.random.uniform(kz, (2,), jnp.float32, 0.0, 1.0)
    loud = 2.0 ** jax.random.uniform(jax.random.fold_in(kz, 1), (), jnp.float32, -1.0, 2.0)
    layers = 2.0 ** jax.random.uniform(kl, (LAYERS, 1, 1), jnp.float32, -1.0, 1.0)
    x = together(ka, jax.random.normal(kx, shape, jnp.float32), much_x) * bump(kf, D, 4.0)
    dy = together(kb, jax.random.normal(kdy, shape, jnp.float32), much_dy)
    drawn = {"x": x.astype(jnp.bfloat16), "dy": (loud * dy * (SEQUENCES * TOKENS) ** -0.5).astype(jnp.bfloat16)}
    for key, name in zip(kw, NAMES, strict=True):
        w = jax.random.normal(key, SHAPES[name], jnp.float32) * SHAPES[name][1] ** -0.5
        drawn[name] = (w * {"w_gate": 1.0, "w_up": bump(kh, FF, 4.0), "w_down": layers}[name]).astype(jnp.bfloat16)
    for key, name in zip(km, NAMES, strict=True):
        drawn[f"m_{name}"] = 0.1 * jax.random.normal(key, SHAPES[name], jnp.float32)
    for key, name in zip(kv, NAMES, strict=True):
        drawn[f"v_{name}"] = jax.random.uniform(key, SHAPES[name], jnp.float32, 0.005, 0.015)
    return drawn


def matmul(a, w):
    return jnp.dot(a, w, preferred_element_type=jnp.float32).astype(jnp.bfloat16)


def normed(h):
    wide = h.astype(jnp.float32)
    scale = lax.rsqrt(jnp.mean(wide**2, -1, keepdims=True) + 1e-6)
    return (wide * scale).astype(jnp.bfloat16)


def layer(h, w):
    a = normed(h)
    gate = jnp.dot(a, w["w_gate"], preferred_element_type=jnp.float32)
    up = jnp.dot(a, w["w_up"], preferred_element_type=jnp.float32)
    return h + matmul((jax.nn.silu(gate) * up).astype(jnp.bfloat16), w["w_down"])


def adamw(w, m, v, g):
    m = 0.9 * m + 0.1 * g
    v = 0.95 * v + 0.05 * g * g
    step = m * lax.rsqrt(v + 1e-8) + 0.1 * w
    return (w - 0.02 * step).astype(jnp.bfloat16), m, v


def stack(weights, h):
    return lax.scan(lambda h, w: (layer(h, w), None), h, weights)[0]


def reference(x, dy, w_gate, w_up, w_down, m_w_gate, m_w_up, m_w_down, v_w_gate, v_w_up, v_w_down):
    weights = dict(zip(NAMES, (w_gate, w_up, w_down), strict=True))

    def take(so_far, sequence):
        h, by_y = sequence
        _, back = jax.vjp(lambda w: stack(w, h), weights)
        return jax.tree.map(lambda total, term: total + term.astype(jnp.float32), so_far, back(by_y)[0]), None

    none_yet = {name: jnp.zeros(w.shape, jnp.float32) for name, w in weights.items()}
    by_weights, _ = lax.scan(take, none_yet, (x, dy))
    gradients = [by_weights[name].astype(jnp.bfloat16).astype(jnp.float32) for name in NAMES]
    new = [
        adamw(w.astype(jnp.float32), m, v, g)
        for w, m, v, g in zip((w_gate, w_up, w_down), (m_w_gate, m_w_up, m_w_down), (v_w_gate, v_w_up, v_w_down), gradients, strict=True)
    ]
    return tuple(one[which] for which in range(3) for one in new)
```

```python
import functools

import jax
import jax.numpy as jnp
from jax import lax
from jax.experimental import pallas as pl
from jax.experimental.pallas import tpu as pltpu
from jax.sharding import PartitionSpec as P


F32, BF16 = jnp.float32, jnp.bfloat16
VMEM_LIMIT = 60 * 1024 * 1024
BN = 256
CROSS = [(i, i ^ 2) for i in range(4)]
INCHIP = [(i, i ^ 1) for i in range(4)]


def params(axes):
    return pltpu.CompilerParams(dimension_semantics=("arbitrary",) * axes, vmem_limit_bytes=VMEM_LIMIT)


def cost(matmuls, elements, moved):
    return pl.CostEstimate(flops=2 * matmuls * elements, bytes_accessed=moved, transcendentals=0)


def dot(a, b, contract):
    return lax.dot_general(a, b, (contract, ((), ())), preferred_element_type=F32)


def normed(h):
    wide = h.astype(F32)
    scale = lax.rsqrt(jnp.mean(wide**2, -1, keepdims=True) + 1e-6)
    return (wide * scale).astype(BF16)


def silu_parts(gate):
    s = jax.nn.sigmoid(gate)
    return gate * s, s + gate * s * (1 - s)


def once(shape, index):
    return pl.BlockSpec(shape, index, pipeline_mode=pl.Buffered(1))


def norm_into(h, a, rows=256):
    def chunk(i, _):
        at = pl.ds(pl.multiple_of(i * rows, rows), rows)
        a[at, :] = normed(h[at, :])

    lax.fori_loop(0, h.shape[0] // rows, chunk, None)


def gates(x, w_gate, w_up, layer, bn=BN):
    t, d = x.shape
    f = w_gate.shape[2]
    n = pl.cdiv(f, bn)

    def body(x, wg, wu, a, gate, up, act):
        @pl.when(pl.program_id(0) == 0)
        def _():
            norm_into(x, a)

        rows = a[...]
        g = dot(rows, wg[...], ((1,), (0,)))
        u = dot(rows, wu[...], ((1,), (0,)))
        gate[...] = g
        up[...] = u
        act[...] = (g * jax.nn.sigmoid(g) * u).astype(BF16)

    return pl.pallas_call(
        body,
        grid=(n,),
        in_specs=[once((t, d), lambda j: (0, 0))] + [pl.BlockSpec((None, d, bn), lambda j: (layer, 0, j))] * 2,
        out_specs=[pl.BlockSpec((t, d), lambda j: (0, 0))]
        + [pl.BlockSpec((None, t, bn), lambda j: (j, 0, 0))] * 2
        + [pl.BlockSpec((t, bn), lambda j: (0, j))],
        out_shape=[jax.ShapeDtypeStruct((t, d), BF16)]
        + [jax.ShapeDtypeStruct((n, t, bn), F32)] * 2
        + [jax.ShapeDtypeStruct((t, f), BF16)],
        compiler_params=params(1),
        cost_estimate=cost(2, t * d * f, 2 * (2 * d * f) + 10 * t * f),
        name="gates",
    )(x, w_gate, w_up)


def down(act, w_down, h, layer, bm=1024, bn=512):
    t, f = act.shape
    d = w_down.shape[2]

    def body(act, w, h, out):
        out[...] = h[...] + dot(act[...], w[...], ((1,), (0,))).astype(BF16)

    return pl.pallas_call(
        body,
        grid=(d // bn, t // bm),
        in_specs=[
            pl.BlockSpec((bm, f), lambda j, i: (i, 0)),
            pl.BlockSpec((None, f, bn), lambda j, i: (layer, 0, j)),
            pl.BlockSpec((bm, bn), lambda j, i: (i, j)),
        ],
        out_specs=pl.BlockSpec((bm, bn), lambda j, i: (i, j)),
        out_shape=jax.ShapeDtypeStruct((t, d), BF16),
        compiler_params=params(2),
        cost_estimate=cost(1, t * d * f, 2 * d * f + 6 * t * f),
        name="down",
    )(act, w_down, h)


def last_layer(h, dy, w_gate, w_up, w_down, layer, bn=BN):
    t, d = h.shape
    f = w_gate.shape[2]

    def body(h, dy, wg, wu, wd, a, act, d_gate, d_up):
        @pl.when(pl.program_id(0) == 0)
        def _():
            norm_into(h, a)

        g = dot(a[...], wg[...], ((1,), (0,)))
        u = dot(a[...], wu[...], ((1,), (0,)))
        da = dot(dy[...], wd[...], ((1,), (1,))).astype(BF16).astype(F32)
        silu, slope = silu_parts(g)
        act[...] = (silu * u).astype(BF16)
        d_gate[...] = (da * u * slope).astype(BF16)
        d_up[...] = (da * silu).astype(BF16)

    return pl.pallas_call(
        body,
        grid=(pl.cdiv(f, bn),),
        in_specs=[once((t, d), lambda j: (0, 0))] * 2
        + [pl.BlockSpec((None, d, bn), lambda j: (layer, 0, j))] * 2
        + [pl.BlockSpec((None, bn, d), lambda j: (layer, j, 0))],
        out_specs=[pl.BlockSpec((t, d), lambda j: (0, 0))] + [pl.BlockSpec((t, bn), lambda j: (0, j))] * 3,
        out_shape=[jax.ShapeDtypeStruct((t, d), BF16)] + [jax.ShapeDtypeStruct((t, f), BF16)] * 3,
        compiler_params=params(1),
        cost_estimate=cost(3, t * d * f, 6 * d * f + 6 * t * f),
        name="last_layer",
    )(h, dy, w_gate, w_up, w_down)


def into_layer(d_gate, d_up, w_gate, w_up, h, dy, layer, bm=256):
    t, f = d_gate.shape
    d = w_gate.shape[1]

    def body(dg, du, wg, wu, h, dy, out):
        by_gate = dot(dg[...], wg[...], ((1,), (1,))).astype(BF16)
        by_up = dot(du[...], wu[...], ((1,), (1,))).astype(BF16)
        by_a = (by_gate.astype(F32) + by_up.astype(F32)).astype(BF16).astype(F32)
        wide = h[...].astype(F32)
        square = jnp.mean(wide**2, -1, keepdims=True) + 1e-6
        scale = lax.rsqrt(square)
        by_square = jnp.sum(by_a * wide, -1, keepdims=True) * (-0.5 * scale / square)
        by_h = (by_a * scale + by_square / d * 2 * wide).astype(BF16)
        out[...] = (dy[...].astype(F32) + by_h.astype(F32)).astype(BF16)

    return pl.pallas_call(
        body,
        grid=(t // bm,),
        in_specs=[pl.BlockSpec((bm, f), lambda i: (i, 0))] * 2
        + [once((None, d, f), lambda i: (layer, 0, 0))] * 2
        + [pl.BlockSpec((bm, d), lambda i: (i, 0))] * 2,
        out_specs=pl.BlockSpec((bm, d), lambda i: (i, 0)),
        out_shape=jax.ShapeDtypeStruct((t, d), BF16),
        compiler_params=params(1),
        cost_estimate=cost(2, t * d * f, 4 * d * f + 4 * t * f),
        name="into_layer",
    )(d_gate, d_up, w_gate, w_up, h, dy)


def to_gates(dh, w_down, gate, up, layer, first, columns, bn=BN):
    t, d = dh.shape

    def body(dh, wd, gate, up, d_gate, d_up):
        da = dot(dh[...], wd[...], ((1,), (1,))).astype(BF16).astype(F32)
        silu, slope = silu_parts(gate[...])
        d_gate[...] = (da * up[...] * slope).astype(BF16)
        d_up[...] = (da * silu).astype(BF16)

    return pl.pallas_call(
        body,
        grid=(pl.cdiv(columns, bn),),
        in_specs=[once((t, d), lambda j: (0, 0)), pl.BlockSpec((None, bn, d), lambda j: (layer, j + first // bn, 0))]
        + [pl.BlockSpec((None, t, bn), lambda j: (j + first // bn, 0, 0))] * 2,
        out_specs=[pl.BlockSpec((t, bn), lambda j: (0, j))] * 2,
        out_shape=[jax.ShapeDtypeStruct((t, columns), BF16)] * 2,
        compiler_params=params(1),
        cost_estimate=cost(1, t * d * columns, 2 * d * columns + 12 * t * columns),
        name="to_gates",
    )(dh, w_down, gate, up)


def weight_gradient(pairs, bm, bn, first=None, rows=None, piece=None):
    k = pairs[0][0].shape[0]
    n = pairs[0][1].shape[1] if piece is None else bn
    skip = 0 if piece is None else piece
    m = pairs[0][0].shape[1] if rows is None else rows
    start = jnp.zeros((1,), jnp.int32) if first is None else (first * (rows // bm)).reshape(1).astype(jnp.int32)
    count = len(pairs)

    def body(start, *refs):
        out = refs[-1]
        total = dot(refs[0][...], refs[1][...], ((0,), (0,)))
        for i in range(1, count):
            total += dot(refs[2 * i][...], refs[2 * i + 1][...], ((0,), (0,)))
        out[...] = total.astype(BF16)

    return pl.pallas_call(
        body,
        grid_spec=pltpu.PrefetchScalarGridSpec(
            num_scalar_prefetch=1,
            grid=(pl.cdiv(n, bn), m // bm),
            in_specs=[
                pl.BlockSpec((k, bm), lambda j, i, s: (0, i + s[0])),
                pl.BlockSpec((k, bn), lambda j, i, s: (0, j + skip)),
            ]
            * count,
            out_specs=pl.BlockSpec((bm, bn), lambda j, i, s: (i, j)),
        ),
        out_shape=jax.ShapeDtypeStruct((m, n), BF16),
        compiler_params=params(2),
        cost_estimate=cost(count, k * m * n, 2 * count * k * (m + n) + 2 * m * n),
        name="weight_gradient",
    )(start, *(t for pair in pairs for t in pair))


def adamw(terms, w, m, v, layer, place, so_far, steps=6):
    _, rows, columns = m.shape
    bm = rows // steps
    arrays, specs, counts = [], [], []
    for run in terms:
        counts.append(len(run))
        for array, entry in run:
            arrays.append(array)
            if entry is None:
                specs.append(pl.BlockSpec((bm, array.shape[-1]), lambda i, s: (i, 0)))
            elif array.ndim == 2:
                specs.append(pl.BlockSpec((bm, array.shape[-1]), lambda i, s, entry=entry: (s[entry] * steps + i, 0)))
            else:
                specs.append(pl.BlockSpec((None, bm, array.shape[-1]), lambda i, s, entry=entry: (s[entry], i, 0)))
    count = len(arrays)

    def body(place, *refs):
        runs, at = [], 0
        for n in counts:
            total = refs[at][...].astype(F32)
            for t in refs[at + 1 : at + n]:
                total += t[...].astype(F32)
            runs.append(total.astype(BF16).astype(F32))
            at += n
        g = jnp.concatenate(runs, 1) if len(runs) > 1 else runs[0]
        w, m, v = (r[...] for r in refs[count : count + 3])
        own, w_out, m_out, v_out = refs[-4:]
        w = w.astype(F32)
        m = 0.9 * m + 0.1 * g
        v = 0.95 * v + 0.05 * g * g
        new = (w - 0.02 * (m * lax.rsqrt(v + 1e-8) + 0.1 * w)).astype(BF16)
        own[...] = new
        w_out[...] = new
        m_out[...] = m
        v_out[...] = v

    plain = pl.BlockSpec((bm, columns), lambda i, s: (i, 0))
    of_w = pl.BlockSpec((None, bm, columns), lambda i, s: (layer, i + s[0] * steps, 0))
    of_m = pl.BlockSpec((None, bm, columns), lambda i, s: (layer, i, 0))
    aliased = [] if so_far is None else list(so_far)
    return pl.pallas_call(
        body,
        grid_spec=pltpu.PrefetchScalarGridSpec(
            num_scalar_prefetch=1,
            grid=(steps,),
            in_specs=specs + [of_w, of_m, of_m] + [pl.BlockSpec(memory_space=pl.ANY)] * len(aliased),
            out_specs=[plain, of_w, of_m, of_m],
        ),
        out_shape=[
            jax.ShapeDtypeStruct((rows, columns), BF16),
            jax.ShapeDtypeStruct(w.shape, BF16),
            jax.ShapeDtypeStruct(m.shape, F32),
            jax.ShapeDtypeStruct(v.shape, F32),
        ],
        input_output_aliases={1 + count + 3 + i: 1 + i for i in range(len(aliased))},
        compiler_params=params(1),
        cost_estimate=pl.CostEstimate(flops=10**9, bytes_accessed=rows * columns * 28, transcendentals=0),
        name="adamw",
    )(place, *arrays, w, m, v, *aliased)


def place(new, blocks, positions, layer, steps=3):
    rows, columns = blocks[0].shape
    bm = rows // steps
    count = len(blocks)

    def body(at, *refs):
        for which in range(count):

            @pl.when(pl.program_id(0) == which)
            def _():
                refs[-1][...] = refs[which][...]

    def of_block(which):
        return pl.BlockSpec((bm, columns), lambda k, i, at: (jnp.where(k == which, i, jnp.where(k < which, 0, steps - 1)), 0))

    return pl.pallas_call(
        body,
        grid_spec=pltpu.PrefetchScalarGridSpec(
            num_scalar_prefetch=1,
            grid=(count, steps),
            in_specs=[of_block(which) for which in range(count)] + [pl.BlockSpec(memory_space=pl.ANY)],
            out_specs=pl.BlockSpec((None, bm, columns), lambda k, i, at: (layer, at[k] * steps + i, 0)),
        ),
        out_shape=jax.ShapeDtypeStruct(new.shape, new.dtype),
        input_output_aliases={count + 1: 0},
        compiler_params=params(2),
        cost_estimate=pl.CostEstimate(flops=10**9, bytes_accessed=4 * count * rows * columns, transcendentals=0),
        name="place",
    )(jnp.stack(positions), *blocks, new)


def step(x, dy, w_gate, w_up, w_down, *moments):
    x, dy = x[0], dy[0]
    index = lax.axis_index("dp").astype(jnp.int32)
    chip, core = index // 2, index % 2

    def across(t):
        return lax.ppermute(t, "dp", CROSS)

    def within(t):
        return lax.ppermute(t, "dp", INCHIP)

    dy_far = across(dy)
    a0, gate0, up0, act0 = gates(x, w_gate, w_up, 0)
    h1 = down(act0, w_down, x, 0)
    h1_far = across(h1)
    a1, act1, d_gate1, d_up1 = last_layer(h1, dy, w_gate, w_up, w_down, 1)
    dh1 = into_layer(d_gate1, d_up1, w_gate, w_up, h1, dy, 1)

    def group_sum(g):
        rows = g.shape[0] // 4
        blocks = g.reshape(2, 2, rows, g.shape[1])
        near = within(lax.dynamic_index_in_dim(blocks, 1 - core, 1, keepdims=False))
        ours = lax.dynamic_index_in_dim(g.reshape(4, rows, g.shape[1]), (1 - chip) * 2 + core, 0, False)
        far = across((ours.astype(F32) + lax.dynamic_index_in_dim(near, 1 - chip, 0, False).astype(F32)).astype(BF16))
        return [(g, 0), (near, 1), (far, None)]

    _, d = x.shape
    f = act0.shape[1]
    terms0 = {name: [] for name in "gud"}
    for number, name in enumerate("abc"):
        g = weight_gradient([(act0, dh1)], 1408, d // 3, piece=number)
        terms0["d"].append(group_sum(g))
    cut = f // 2 // BN * BN
    for first, columns, bn in ((0, cut, 512), (cut, f - cut, 768)):
        d_gate0, d_up0 = to_gates(dh1, w_down, gate0, up0, 0, first, columns)
        g = weight_gradient([(a0, d_gate0)], d, bn)
        terms0["g"].append(group_sum(g))
        g = weight_gradient([(a0, d_up0)], d, bn)
        terms0["u"].append(group_sum(g))

    h1_far, _ = lax.optimization_barrier((h1_far, g))
    a1_far, act1_far, d_gate1_far, d_up1_far = last_layer(h1_far, dy_far, w_gate, w_up, w_down, 1)
    act1, act1_far = lax.optimization_barrier((act1, act1_far))
    lanes = f // 2 // 128 * 128
    columns_of = functools.partial(lax.dynamic_slice_in_dim, start_index=chip * lanes, slice_size=f - lanes, axis=1)
    g_down1 = weight_gradient([(columns_of(act1), dy), (columns_of(act1_far), dy_far)], f - lanes, 512)
    half = d // 2
    g_gate1 = weight_gradient([(a1, d_gate1), (a1_far, d_gate1_far)], half, 512, chip, half)
    g_up1 = weight_gradient([(a1, d_up1), (a1_far, d_up1_far)], half, 512, chip, half)

    def of_the_chip(g, rows, offset=None):
        start = 0 if offset is None else offset
        near = within(lax.dynamic_slice_in_dim(g, start + (1 - core) * rows, rows, 0))
        ours = (g, 2) if offset is None else (lax.dynamic_slice_in_dim(g, start + core * rows, rows, 0), None)
        return [[ours, (near, None)]]

    terms1 = {
        "g": of_the_chip(g_gate1, half // 2),
        "u": of_the_chip(g_up1, half // 2),
        "d": of_the_chip(g_down1, f // 4, chip * (f // 2 - lanes)),
    }

    here = jnp.stack([index, chip, core])
    at_near, at_far, at_newer = chip * 2 + 1 - core, (1 - chip) * 2 + core, (1 - chip) * 2 + 1 - core
    new = []
    for which, name in enumerate("gud"):
        w, m, v = (w_gate, w_up, w_down)[which], moments[which], moments[3 + which]
        own0, *so_far = adamw(terms0[name], w, m, v, 0, here, None)
        own1, w_new, m_new, v_new = adamw(terms1[name], w, m, v, 1, here, so_far)
        for layer, own in ((0, own0), (1, own1)):
            label = name + str(layer)
            near = within(own)
            if label != "d1":
                far = across(own)
                newer = within(far)
                w_new = place(w_new, (near, far, newer), (at_near, at_far, at_newer), layer)
                continue
            rows = own.shape[0] // 2
            far = [across(own[part * rows :][:rows]) for part in (0, 1)]
            newer = [within(t) for t in far]
            w_new = place(w_new, (near,), (at_near,), layer)
            w_new = place(w_new, (far[0], newer[0]), (at_far * 2, at_newer * 2), layer)
            w_new = place(w_new, (far[1],), (at_far * 2 + 1,), layer)
            w_new = place(w_new, (newer[1],), (at_newer * 2 + 1,), layer)
        new.append((w_new, m_new, v_new))
    return tuple(one[which] for which in range(3) for one in new)


def solution(mesh):
    sequences, whole, rows, group = P(("rep", "dp")), P(), P(None, "dp"), P("rep")

    return jax.shard_map(
        step,
        mesh=mesh,
        in_specs=(sequences,) * 2 + (whole,) * 3 + (rows,) * 6,
        out_specs=(group,) * 3 + (P("rep", "dp"),) * 6,
        check_vma=False,
    )
```

```python
import jax
import jax.numpy as jnp
from jax import lax
from jax.experimental import pallas as pl
from jax.experimental.pallas import tpu as pltpu
from jax.sharding import PartitionSpec as P


F32, BF16 = jnp.float32, jnp.bfloat16
VMEM_LIMIT = 60 * 1024 * 1024
BN = 256
CROSS = [(i, i ^ 2) for i in range(4)]
INCHIP = [(i, i ^ 1) for i in range(4)]


def params(axes):
    return pltpu.CompilerParams(dimension_semantics=("arbitrary",) * axes, vmem_limit_bytes=VMEM_LIMIT)


def cost(matmuls, elements, moved):
    return pl.CostEstimate(flops=2 * matmuls * elements, bytes_accessed=moved, transcendentals=0)


def dot(a, b, contract):
    return lax.dot_general(a, b, (contract, ((), ())), preferred_element_type=F32)


def normed(h):
    wide = h.astype(F32)
    scale = lax.rsqrt(jnp.mean(wide**2, -1, keepdims=True) + 1e-6)
    return (wide * scale).astype(BF16)


def silu_parts(gate):
    s = jax.nn.sigmoid(gate)
    return gate * s, s + gate * s * (1 - s)


def once(shape, index):
    return pl.BlockSpec(shape, index, pipeline_mode=pl.Buffered(1))


def parts(n, count=4):
    return [pl.ds(i * (n // count), n // count) for i in range(count)]


def norm_into(h, a, rows=256):
    def chunk(i, _):
        at = pl.ds(pl.multiple_of(i * rows, rows), rows)
        a[at, :] = normed(h[at, :])

    lax.fori_loop(0, h.shape[0] // rows, chunk, None)


def gates(x, w_gate, w_up, layer, bn=BN):
    t, d = x.shape
    f = w_gate.shape[2]
    n = pl.cdiv(f, bn)

    def body(x, wg, wu, a, gate, up, act):
        @pl.when(pl.program_id(0) == 0)
        def _():
            norm_into(x, a)

        for at in parts(t):
            g = dot(a[at, :], wg[...], ((1,), (0,)))
            u = dot(a[at, :], wu[...], ((1,), (0,)))
            gate[at, :] = g
            up[at, :] = u
            act[at, :] = (g * jax.nn.sigmoid(g) * u).astype(BF16)

    return pl.pallas_call(
        body,
        grid=(n,),
        in_specs=[once((t, d), lambda j: (0, 0))] + [pl.BlockSpec((None, d, bn), lambda j: (layer, 0, j))] * 2,
        out_specs=[pl.BlockSpec((t, d), lambda j: (0, 0))]
        + [pl.BlockSpec((None, t, bn), lambda j: (j, 0, 0))] * 2
        + [pl.BlockSpec((t, bn), lambda j: (0, j))],
        out_shape=[jax.ShapeDtypeStruct((t, d), BF16)]
        + [jax.ShapeDtypeStruct((n, t, bn), F32)] * 2
        + [jax.ShapeDtypeStruct((t, f), BF16)],
        compiler_params=params(1),
        cost_estimate=cost(2, t * d * f, 2 * (2 * d * f) + 10 * t * f),
        name="gates",
    )(x, w_gate, w_up)


def down(act, w_down, h, layer, bm=1024, bn=512):
    t, f = act.shape
    d = w_down.shape[2]

    def body(act, w, h, out):
        out[...] = h[...] + dot(act[...], w[...], ((1,), (0,))).astype(BF16)

    return pl.pallas_call(
        body,
        grid=(d // bn, t // bm),
        in_specs=[
            pl.BlockSpec((bm, f), lambda j, i: (i, 0)),
            pl.BlockSpec((None, f, bn), lambda j, i: (layer, 0, j)),
            pl.BlockSpec((bm, bn), lambda j, i: (i, j)),
        ],
        out_specs=pl.BlockSpec((bm, bn), lambda j, i: (i, j)),
        out_shape=jax.ShapeDtypeStruct((t, d), BF16),
        compiler_params=params(2),
        cost_estimate=cost(1, t * d * f, 2 * d * f + 6 * t * f),
        name="down",
    )(act, w_down, h)


def last_layer(h, dy, w_gate, w_up, w_down, layer, chip, kept, bn=BN):
    t, d = h.shape
    f = w_gate.shape[2]
    skip = f // 2 // bn
    wanted = pl.cdiv(kept, bn)

    def body(chip, h, dy, wg, wu, wd, a, act, d_gate, d_up):
        @pl.when(pl.program_id(0) == 0)
        def _():
            norm_into(h, a)

        for at in parts(t):
            g = dot(a[at, :], wg[...], ((1,), (0,)))
            u = dot(a[at, :], wu[...], ((1,), (0,)))
            da = dot(dy[at, :], wd[...], ((1,), (1,))).astype(BF16).astype(F32)
            silu, slope = silu_parts(g)
            act[at, :] = (silu * u).astype(BF16)
            d_gate[at, :] = (da * u * slope).astype(BF16)
            d_up[at, :] = (da * silu).astype(BF16)

    def act_block(j, s):
        at = j - s[0] * skip
        return 0, jnp.where(jnp.logical_and(at >= 0, at < wanted), at, wanted)

    return pl.pallas_call(
        body,
        grid_spec=pltpu.PrefetchScalarGridSpec(
            num_scalar_prefetch=1,
            grid=(pl.cdiv(f, bn),),
            in_specs=[once((t, d), lambda j, s: (0, 0))] * 2
            + [pl.BlockSpec((None, d, bn), lambda j, s: (layer, 0, j))] * 2
            + [pl.BlockSpec((None, bn, d), lambda j, s: (layer, j, 0))],
            out_specs=[
                pl.BlockSpec((t, d), lambda j, s: (0, 0)),
                pl.BlockSpec((t, bn), act_block),
            ]
            + [pl.BlockSpec((t, bn), lambda j, s: (0, j))] * 2,
        ),
        out_shape=[jax.ShapeDtypeStruct((t, d), BF16), jax.ShapeDtypeStruct((t, (wanted + 1) * bn), BF16)]
        + [jax.ShapeDtypeStruct((t, f), BF16)] * 2,
        compiler_params=params(1),
        cost_estimate=cost(3, t * d * f, 6 * d * f + 6 * t * f),
        name="last_layer",
    )(chip.reshape(1), h, dy, w_gate, w_up, w_down)


def into_layer(d_gate, d_up, w_gate, w_up, h, dy, layer, bm=256):
    t, f = d_gate.shape
    d = w_gate.shape[1]

    def body(dg, du, wg, wu, h, dy, out):
        by_gate = dot(dg[...], wg[...], ((1,), (1,))).astype(BF16)
        by_up = dot(du[...], wu[...], ((1,), (1,))).astype(BF16)
        by_a = (by_gate.astype(F32) + by_up.astype(F32)).astype(BF16).astype(F32)
        wide = h[...].astype(F32)
        square = jnp.mean(wide**2, -1, keepdims=True) + 1e-6
        scale = lax.rsqrt(square)
        by_square = jnp.sum(by_a * wide, -1, keepdims=True) * (-0.5 * scale / square)
        by_h = (by_a * scale + by_square / d * 2 * wide).astype(BF16)
        out[...] = (dy[...].astype(F32) + by_h.astype(F32)).astype(BF16)

    return pl.pallas_call(
        body,
        grid=(t // bm,),
        in_specs=[pl.BlockSpec((bm, f), lambda i: (i, 0))] * 2
        + [once((None, d, f), lambda i: (layer, 0, 0))] * 2
        + [pl.BlockSpec((bm, d), lambda i: (i, 0))] * 2,
        out_specs=pl.BlockSpec((bm, d), lambda i: (i, 0)),
        out_shape=jax.ShapeDtypeStruct((t, d), BF16),
        compiler_params=params(1),
        cost_estimate=cost(2, t * d * f, 4 * d * f + 4 * t * f),
        name="into_layer",
    )(d_gate, d_up, w_gate, w_up, h, dy)


def to_gates(dh, w_down, gate, up, layer, first, columns, bn=BN):
    t, d = dh.shape

    def body(dh, wd, gate, up, d_gate, d_up):
        for block in range(2):
            columns_at = pl.ds(block * bn, bn)
            for at in parts(t):
                da = dot(dh[at, :], wd[columns_at, :], ((1,), (1,))).astype(BF16).astype(F32)
                silu, slope = silu_parts(gate[block, at, :])
                d_gate[at, columns_at] = (da * up[block, at, :] * slope).astype(BF16)
                d_up[at, columns_at] = (da * silu).astype(BF16)

    skip = first // (2 * bn)
    return pl.pallas_call(
        body,
        grid=(pl.cdiv(columns, 2 * bn),),
        in_specs=[once((t, d), lambda j: (0, 0)), pl.BlockSpec((None, 2 * bn, d), lambda j: (layer, j + skip, 0))]
        + [pl.BlockSpec((2, t, bn), lambda j: (j + skip, 0, 0))] * 2,
        out_specs=[pl.BlockSpec((t, 2 * bn), lambda j: (0, j))] * 2,
        out_shape=[jax.ShapeDtypeStruct((t, columns), BF16)] * 2,
        compiler_params=params(1),
        cost_estimate=cost(1, t * d * columns, 2 * d * columns + 12 * t * columns),
        name="to_gates",
    )(dh, w_down, gate, up)


def weight_gradient(pairs, bm, bn, first=None, rows=None, piece=None):
    k = pairs[0][0].shape[0]
    n = pairs[0][1].shape[1] if piece is None else bn
    skip = 0 if piece is None else piece
    m = pairs[0][0].shape[1] if rows is None else rows
    start = jnp.zeros((1,), jnp.int32) if first is None else (first * (rows // bm)).reshape(1).astype(jnp.int32)
    count = len(pairs)

    def body(start, *refs):
        out = refs[-1]
        total = dot(refs[0][...], refs[1][...], ((0,), (0,)))
        for i in range(1, count):
            total += dot(refs[2 * i][...], refs[2 * i + 1][...], ((0,), (0,)))
        out[...] = total.astype(BF16)

    return pl.pallas_call(
        body,
        grid_spec=pltpu.PrefetchScalarGridSpec(
            num_scalar_prefetch=1,
            grid=(pl.cdiv(n, bn), m // bm),
            in_specs=[
                pl.BlockSpec((k, bm), lambda j, i, s: (0, i + s[0])),
                pl.BlockSpec((k, bn), lambda j, i, s: (0, j + skip)),
            ]
            * count,
            out_specs=pl.BlockSpec((bm, bn), lambda j, i, s: (i, j)),
        ),
        out_shape=jax.ShapeDtypeStruct((m, n), BF16),
        compiler_params=params(2),
        cost_estimate=cost(count, k * m * n, 2 * count * k * (m + n) + 2 * m * n),
        name="weight_gradient",
    )(start, *(t for pair in pairs for t in pair))


def adamw(terms, w, m, v, layer, place, so_far, steps=6):
    _, rows, columns = m.shape
    bm = rows // steps
    arrays, specs, counts = [], [], []
    for run in terms:
        counts.append(len(run))
        for array, entry in run:
            arrays.append(array)
            if entry is None:
                specs.append(pl.BlockSpec((bm, array.shape[-1]), lambda i, s: (i, 0)))
            elif array.ndim == 2:
                specs.append(pl.BlockSpec((bm, array.shape[-1]), lambda i, s, entry=entry: (s[entry] * steps + i, 0)))
            else:
                specs.append(pl.BlockSpec((None, bm, array.shape[-1]), lambda i, s, entry=entry: (s[entry], i, 0)))
    count = len(arrays)

    def body(place, *refs):
        runs, at = [], 0
        for n in counts:
            total = refs[at][...].astype(F32)
            for t in refs[at + 1 : at + n]:
                total += t[...].astype(F32)
            runs.append(total.astype(BF16).astype(F32))
            at += n
        g = jnp.concatenate(runs, 1) if len(runs) > 1 else runs[0]
        w, m, v = (r[...] for r in refs[count : count + 3])
        own, w_out, m_out, v_out = refs[-4:]
        w = w.astype(F32)
        m = 0.9 * m + 0.1 * g
        v = 0.95 * v + 0.05 * g * g
        new = (w - 0.02 * (m * lax.rsqrt(v + 1e-8) + 0.1 * w)).astype(BF16)
        own[...] = new
        w_out[...] = new
        m_out[...] = m
        v_out[...] = v

    plain = pl.BlockSpec((bm, columns), lambda i, s: (i, 0))
    of_w = pl.BlockSpec((None, bm, columns), lambda i, s: (layer, i + s[0] * steps, 0))
    of_m = pl.BlockSpec((None, bm, columns), lambda i, s: (layer, i, 0))
    aliased = [] if so_far is None else list(so_far)
    return pl.pallas_call(
        body,
        grid_spec=pltpu.PrefetchScalarGridSpec(
            num_scalar_prefetch=1,
            grid=(steps,),
            in_specs=specs + [of_w, of_m, of_m] + [pl.BlockSpec(memory_space=pl.ANY)] * len(aliased),
            out_specs=[plain, of_w, of_m, of_m],
        ),
        out_shape=[
            jax.ShapeDtypeStruct((rows, columns), BF16),
            jax.ShapeDtypeStruct(w.shape, BF16),
            jax.ShapeDtypeStruct(m.shape, F32),
            jax.ShapeDtypeStruct(v.shape, F32),
        ],
        input_output_aliases={1 + count + 3 + i: 1 + i for i in range(len(aliased))},
        compiler_params=params(1),
        cost_estimate=pl.CostEstimate(flops=10**9, bytes_accessed=rows * columns * 28, transcendentals=0),
        name="adamw",
    )(place, *arrays, w, m, v, *aliased)


def place(new, blocks, positions, layer, steps=3):
    rows, columns = blocks[0].shape
    bm = rows // steps
    count = len(blocks)

    def body(at, *refs):
        for which in range(count):

            @pl.when(pl.program_id(0) == which)
            def _():
                refs[-1][...] = refs[which][...]

    def of_block(which):
        return pl.BlockSpec((bm, columns), lambda k, i, at: (jnp.where(k == which, i, jnp.where(k < which, 0, steps - 1)), 0))

    return pl.pallas_call(
        body,
        grid_spec=pltpu.PrefetchScalarGridSpec(
            num_scalar_prefetch=1,
            grid=(count, steps),
            in_specs=[of_block(which) for which in range(count)] + [pl.BlockSpec(memory_space=pl.ANY)],
            out_specs=pl.BlockSpec((None, bm, columns), lambda k, i, at: (layer, at[k] * steps + i, 0)),
        ),
        out_shape=jax.ShapeDtypeStruct(new.shape, new.dtype),
        input_output_aliases={count + 1: 0},
        compiler_params=params(2),
        cost_estimate=pl.CostEstimate(flops=10**9, bytes_accessed=4 * count * rows * columns, transcendentals=0),
        name="place",
    )(jnp.stack(positions), *blocks, new)


def step(x, dy, w_gate, w_up, w_down, *moments):
    x, dy = x[0], dy[0]
    index = lax.axis_index("dp").astype(jnp.int32)
    chip, core = index // 2, index % 2

    def across(t):
        return lax.ppermute(t, "dp", CROSS)

    def within(t):
        return lax.ppermute(t, "dp", INCHIP)

    dy_far = across(dy)
    a0, gate0, up0, act0 = gates(x, w_gate, w_up, 0)
    h1 = down(act0, w_down, x, 0)
    f = act0.shape[1]
    kept = f - f // 2 // BN * BN
    h1_far = across(h1)
    a1, act1, d_gate1, d_up1 = last_layer(h1, dy, w_gate, w_up, w_down, 1, chip, kept)
    dh1 = into_layer(d_gate1, d_up1, w_gate, w_up, h1, dy, 1)

    def group_sum(g, whole=True):
        rows = g.shape[0] // 4
        blocks = g.reshape(4, rows, g.shape[1])
        far_block = (1 - chip) * 2 + core
        if whole:
            near = within(g)
            theirs = lax.dynamic_index_in_dim(near.reshape(blocks.shape), far_block, 0, False)
        else:
            near = within(lax.dynamic_index_in_dim(g.reshape(2, 2, rows, g.shape[1]), 1 - core, 1, keepdims=False))
            theirs = lax.dynamic_index_in_dim(near, 1 - chip, 0, False)
        ours = lax.dynamic_index_in_dim(blocks, far_block, 0, False)
        far = across((ours.astype(F32) + theirs.astype(F32)).astype(BF16))
        return [(g, 0), (near, 0 if whole else 1), (far, None)]

    _, d = x.shape
    terms0 = {name: [] for name in "gud"}
    for number, name in enumerate("abc"):
        g = weight_gradient([(act0, dh1)], 1408, d // 3, piece=number)
        terms0["d"].append(group_sum(g, name != "c"))
    cut = f // 2 // BN * BN
    for name, first, columns, bn in (("a", 0, cut, 512), ("b", cut, f - cut, 768)):
        d_gate0, d_up0 = to_gates(dh1, w_down, gate0, up0, 0, first, columns)
        g = weight_gradient([(a0, d_gate0)], d, bn)
        terms0["g"].append(group_sum(g, name != "a"))
        g = weight_gradient([(a0, d_up0)], d, bn)
        terms0["u"].append(group_sum(g))

    h1_far, _ = lax.optimization_barrier((h1_far, g))
    a1_far, act1_far, d_gate1_far, d_up1_far = last_layer(h1_far, dy_far, w_gate, w_up, w_down, 1, chip, kept)
    g_down1 = weight_gradient([(act1, dy), (act1_far, dy_far)], kept, 512, None, kept)
    half = d // 2
    g_gate1 = weight_gradient([(a1, d_gate1), (a1_far, d_gate1_far)], half, 512, chip, half)
    g_up1 = weight_gradient([(a1, d_up1), (a1_far, d_up1_far)], half, 512, chip, half)

    def of_the_chip(g, rows, offset=None):
        start = 0 if offset is None else offset
        near = within(lax.dynamic_slice_in_dim(g, start + (1 - core) * rows, rows, 0))
        ours = (g, 2) if offset is None else (lax.dynamic_slice_in_dim(g, start + core * rows, rows, 0), None)
        return [[ours, (near, None)]]

    terms1 = {
        "g": of_the_chip(g_gate1, half // 2),
        "u": of_the_chip(g_up1, half // 2),
        "d": of_the_chip(g_down1, f // 4, chip * (f // 2 - (f - kept))),
    }

    here = jnp.stack([index, chip, core])
    at_near, at_far, at_newer = chip * 2 + 1 - core, (1 - chip) * 2 + core, (1 - chip) * 2 + 1 - core
    new = []
    for which, name in enumerate("gud"):
        w, m, v = (w_gate, w_up, w_down)[which], moments[which], moments[3 + which]
        own0, *so_far = adamw(terms0[name], w, m, v, 0, here, None)
        own1, w_new, m_new, v_new = adamw(terms1[name], w, m, v, 1, here, so_far)
        for layer, own in ((0, own0), (1, own1)):
            label = name + str(layer)
            near = within(own)
            if label != "d1":
                far = across(own)
                newer = within(far)
                w_new = place(w_new, (near, far, newer), (at_near, at_far, at_newer), layer)
                continue
            rows = own.shape[0] // 2
            far = [across(own[part * rows :][:rows]) for part in (0, 1)]
            newer = [within(t) for t in far]
            w_new = place(w_new, (near,), (at_near,), layer)
            w_new = place(w_new, (far[0], newer[0]), (at_far * 2, at_newer * 2), layer)
            w_new = place(w_new, (far[1],), (at_far * 2 + 1,), layer)
            w_new = place(w_new, (newer[1],), (at_newer * 2 + 1,), layer)
        new.append((w_new, m_new, v_new))
    return tuple(one[which] for which in range(3) for one in new)


def solution(mesh):
    sequences, whole, rows, group = P(("rep", "dp")), P(), P(None, "dp"), P("rep")

    return jax.shard_map(
        step,
        mesh=mesh,
        in_specs=(sequences,) * 2 + (whole,) * 3 + (rows,) * 6,
        out_specs=(group,) * 3 + (P("rep", "dp"),) * 6,
        check_vma=False,
    )
```

```python
import jax
import jax.numpy as jnp
from jax import lax
from jax.experimental import pallas as pl
from jax.experimental.pallas import tpu as pltpu
from jax.sharding import PartitionSpec as P


F32, BF16 = jnp.float32, jnp.bfloat16
VMEM_LIMIT = 60 * 1024 * 1024
BN = 256
CROSS = [(i, i ^ 2) for i in range(4)]
INCHIP = [(i, i ^ 1) for i in range(4)]


def params(axes):
    return pltpu.CompilerParams(dimension_semantics=("arbitrary",) * axes, vmem_limit_bytes=VMEM_LIMIT)


def cost(matmuls, elements, moved):
    return pl.CostEstimate(flops=2 * matmuls * elements, bytes_accessed=moved, transcendentals=0)


def dot(a, b, contract):
    return lax.dot_general(a, b, (contract, ((), ())), preferred_element_type=F32)


def normed(h):
    wide = h.astype(F32)
    scale = lax.rsqrt(jnp.mean(wide**2, -1, keepdims=True) + 1e-6)
    return (wide * scale).astype(BF16)


def silu_parts(gate):
    s = jax.nn.sigmoid(gate)
    return gate * s, s + gate * s * (1 - s)


def once(shape, index):
    return pl.BlockSpec(shape, index, pipeline_mode=pl.Buffered(1))


def parts(n, count=4):
    return [pl.ds(i * (n // count), n // count) for i in range(count)]


def norm_into(h, a, rows=256):
    def chunk(i, _):
        at = pl.ds(pl.multiple_of(i * rows, rows), rows)
        a[at, :] = normed(h[at, :])

    lax.fori_loop(0, h.shape[0] // rows, chunk, None)


def gates(x, w_gate, w_up, layer, bn=BN):
    t, d = x.shape
    f = w_gate.shape[2]
    n = pl.cdiv(f, bn)

    def body(x, wg, wu, a, gate, up, act):
        @pl.when(pl.program_id(0) == 0)
        def _():
            norm_into(x, a)

        for at in parts(t):
            g = dot(a[at, :], wg[...], ((1,), (0,)))
            u = dot(a[at, :], wu[...], ((1,), (0,)))
            gate[at, :] = g
            up[at, :] = u
            act[at, :] = (g * jax.nn.sigmoid(g) * u).astype(BF16)

    return pl.pallas_call(
        body,
        grid=(n,),
        in_specs=[once((t, d), lambda j: (0, 0))] + [pl.BlockSpec((None, d, bn), lambda j: (layer, 0, j))] * 2,
        out_specs=[pl.BlockSpec((t, d), lambda j: (0, 0))]
        + [pl.BlockSpec((None, t, bn), lambda j: (j, 0, 0))] * 2
        + [pl.BlockSpec((t, bn), lambda j: (0, j))],
        out_shape=[jax.ShapeDtypeStruct((t, d), BF16)]
        + [jax.ShapeDtypeStruct((n, t, bn), F32)] * 2
        + [jax.ShapeDtypeStruct((t, f), BF16)],
        compiler_params=params(1),
        cost_estimate=cost(2, t * d * f, 2 * (2 * d * f) + 10 * t * f),
        name="gates",
    )(x, w_gate, w_up)


def down(act, w_down, h, layer, bm=1024, bn=512):
    t, f = act.shape
    d = w_down.shape[2]

    def body(act, w, h, out):
        out[...] = h[...] + dot(act[...], w[...], ((1,), (0,))).astype(BF16)

    return pl.pallas_call(
        body,
        grid=(d // bn, t // bm),
        in_specs=[
            pl.BlockSpec((bm, f), lambda j, i: (i, 0)),
            pl.BlockSpec((None, f, bn), lambda j, i: (layer, 0, j)),
            pl.BlockSpec((bm, bn), lambda j, i: (i, j)),
        ],
        out_specs=pl.BlockSpec((bm, bn), lambda j, i: (i, j)),
        out_shape=jax.ShapeDtypeStruct((t, d), BF16),
        compiler_params=params(2),
        cost_estimate=cost(1, t * d * f, 2 * d * f + 6 * t * f),
        name="down",
    )(act, w_down, h)


def last_layer(h, dy, w_gate, w_up, w_down, layer, chip, kept, bn=BN):
    t, d = h.shape
    f = w_gate.shape[2]
    skip = f // 2 // bn
    wanted = pl.cdiv(kept, bn)

    def body(chip, h, dy, wg, wu, wd, a, act, d_gate, d_up):
        @pl.when(pl.program_id(0) == 0)
        def _():
            norm_into(h, a)

        for at in parts(t):
            g = dot(a[at, :], wg[...], ((1,), (0,)))
            u = dot(a[at, :], wu[...], ((1,), (0,)))
            da = dot(dy[at, :], wd[...], ((1,), (1,))).astype(BF16).astype(F32)
            silu, slope = silu_parts(g)
            act[at, :] = (silu * u).astype(BF16)
            d_gate[at, :] = (da * u * slope).astype(BF16)
            d_up[at, :] = (da * silu).astype(BF16)

    def act_block(j, s):
        at = j - s[0] * skip
        return 0, jnp.where(jnp.logical_and(at >= 0, at < wanted), at, wanted)

    return pl.pallas_call(
        body,
        grid_spec=pltpu.PrefetchScalarGridSpec(
            num_scalar_prefetch=1,
            grid=(pl.cdiv(f, bn),),
            in_specs=[once((t, d), lambda j, s: (0, 0))] * 2
            + [pl.BlockSpec((None, d, bn), lambda j, s: (layer, 0, j))] * 2
            + [pl.BlockSpec((None, bn, d), lambda j, s: (layer, j, 0))],
            out_specs=[
                pl.BlockSpec((t, d), lambda j, s: (0, 0)),
                pl.BlockSpec((t, bn), act_block),
            ]
            + [pl.BlockSpec((t, bn), lambda j, s: (0, j))] * 2,
        ),
        out_shape=[jax.ShapeDtypeStruct((t, d), BF16), jax.ShapeDtypeStruct((t, (wanted + 1) * bn), BF16)]
        + [jax.ShapeDtypeStruct((t, f), BF16)] * 2,
        compiler_params=params(1),
        cost_estimate=cost(3, t * d * f, 6 * d * f + 6 * t * f),
        name="last_layer",
    )(chip.reshape(1), h, dy, w_gate, w_up, w_down)


def into_layer(d_gate, d_up, w_gate, w_up, h, dy, layer, bm=256):
    t, f = d_gate.shape
    d = w_gate.shape[1]

    steps = t // bm

    def body(dg, du, wg, wu, h, dy, out, w_up, by_gate, done):
        step = pl.program_id(1)
        at = pl.ds(pl.multiple_of(step * bm, bm), bm)
        fetch = pltpu.make_async_copy(wu.at[layer], w_up, done)

        @pl.when(pl.program_id(0) == 0)
        def _():
            @pl.when(step == 0)
            def _():
                fetch.start()

            by_gate[at, :] = dot(dg[...], wg[...], ((1,), (1,))).astype(BF16)

        @pl.when(pl.program_id(0) == 1)
        def _():
            @pl.when(step == 0)
            def _():
                fetch.wait()

            by_up = dot(du[...], w_up[...], ((1,), (1,))).astype(BF16)
            by_a = (by_gate[at, :].astype(F32) + by_up.astype(F32)).astype(BF16).astype(F32)
            wide = h[...].astype(F32)
            square = jnp.mean(wide**2, -1, keepdims=True) + 1e-6
            scale = lax.rsqrt(square)
            by_square = jnp.sum(by_a * wide, -1, keepdims=True) * (-0.5 * scale / square)
            by_h = (by_a * scale + by_square / d * 2 * wide).astype(BF16)
            out[...] = (dy[...].astype(F32) + by_h.astype(F32)).astype(BF16)

    def second(p, i):
        return i * p, 0

    return pl.pallas_call(
        body,
        grid=(2, steps),
        in_specs=[
            pl.BlockSpec((bm, f), lambda p, i: (i + (steps - 1 - i) * p, 0)),
            pl.BlockSpec((bm, f), second),
            once((None, d, f), lambda p, i: (layer, 0, 0)),
            pl.BlockSpec(memory_space=pl.ANY),
            pl.BlockSpec((bm, d), second),
            pl.BlockSpec((bm, d), second),
        ],
        out_specs=pl.BlockSpec((bm, d), second),
        out_shape=jax.ShapeDtypeStruct((t, d), BF16),
        scratch_shapes=[pltpu.VMEM((d, f), BF16), pltpu.VMEM((t, d), BF16), pltpu.SemaphoreType.DMA],
        compiler_params=params(2),
        cost_estimate=cost(2, t * d * f, 4 * d * f + 4 * t * f),
        name="into_layer",
    )(d_gate, d_up, w_gate, w_up, h, dy)


def to_gates(dh, w_down, gate, up, layer, first, columns, bn=BN):
    t, d = dh.shape

    def body(dh, wd, gate, up, d_gate, d_up):
        for at in parts(t):
            da = dot(dh[at, :], wd[...], ((1,), (1,))).astype(BF16).astype(F32)
            silu, slope = silu_parts(gate[at, :])
            d_gate[at, :] = (da * up[at, :] * slope).astype(BF16)
            d_up[at, :] = (da * silu).astype(BF16)

    skip = first // bn
    return pl.pallas_call(
        body,
        grid=(pl.cdiv(columns, bn),),
        in_specs=[once((t, d), lambda j: (0, 0)), pl.BlockSpec((None, bn, d), lambda j: (layer, j + skip, 0))]
        + [pl.BlockSpec((None, t, bn), lambda j: (j + skip, 0, 0))] * 2,
        out_specs=[pl.BlockSpec((t, bn), lambda j: (0, j))] * 2,
        out_shape=[jax.ShapeDtypeStruct((t, columns), BF16)] * 2,
        compiler_params=params(1),
        cost_estimate=cost(1, t * d * columns, 2 * d * columns + 12 * t * columns),
        name="to_gates",
    )(dh, w_down, gate, up)


def weight_gradient(pairs, bm, bn, first=None, rows=None, piece=None):
    k = pairs[0][0].shape[0]
    n = pairs[0][1].shape[1] if piece is None else bn
    skip = 0 if piece is None else piece
    m = pairs[0][0].shape[1] if rows is None else rows
    start = jnp.zeros((1,), jnp.int32) if first is None else (first * (rows // bm)).reshape(1).astype(jnp.int32)
    count = len(pairs)

    def body(start, *refs):
        out = refs[-1]
        total = dot(refs[0][...], refs[1][...], ((0,), (0,)))
        for i in range(1, count):
            total += dot(refs[2 * i][...], refs[2 * i + 1][...], ((0,), (0,)))
        out[...] = total.astype(BF16)

    return pl.pallas_call(
        body,
        grid_spec=pltpu.PrefetchScalarGridSpec(
            num_scalar_prefetch=1,
            grid=(pl.cdiv(n, bn), m // bm),
            in_specs=[
                pl.BlockSpec((k, bm), lambda j, i, s: (0, i + s[0])),
                pl.BlockSpec((k, bn), lambda j, i, s: (0, j + skip)),
            ]
            * count,
            out_specs=pl.BlockSpec((bm, bn), lambda j, i, s: (i, j)),
        ),
        out_shape=jax.ShapeDtypeStruct((m, n), BF16),
        compiler_params=params(2),
        cost_estimate=cost(count, k * m * n, 2 * count * k * (m + n) + 2 * m * n),
        name="weight_gradient",
    )(start, *(t for pair in pairs for t in pair))


def adamw(terms, w, m, v, layer, place, so_far, steps=6):
    _, rows, columns = m.shape
    bm = rows // steps
    arrays, specs, counts = [], [], []
    for run in terms:
        counts.append(len(run))
        for array, entry in run:
            arrays.append(array)
            if entry is None:
                specs.append(pl.BlockSpec((bm, array.shape[-1]), lambda i, s: (i, 0)))
            elif array.ndim == 2:
                specs.append(pl.BlockSpec((bm, array.shape[-1]), lambda i, s, entry=entry: (s[entry] * steps + i, 0)))
            else:
                specs.append(pl.BlockSpec((None, bm, array.shape[-1]), lambda i, s, entry=entry: (s[entry], i, 0)))
    count = len(arrays)

    def body(place, *refs):
        runs, at = [], 0
        for n in counts:
            total = refs[at][...].astype(F32)
            for t in refs[at + 1 : at + n]:
                total += t[...].astype(F32)
            runs.append(total.astype(BF16).astype(F32))
            at += n
        g = jnp.concatenate(runs, 1) if len(runs) > 1 else runs[0]
        w, m, v = (r[...] for r in refs[count : count + 3])
        own, w_out, m_out, v_out = refs[-4:]
        w = w.astype(F32)
        m = 0.9 * m + 0.1 * g
        v = 0.95 * v + 0.05 * g * g
        new = (w - 0.02 * (m * lax.rsqrt(v + 1e-8) + 0.1 * w)).astype(BF16)
        own[...] = new
        w_out[...] = new
        m_out[...] = m
        v_out[...] = v

    plain = pl.BlockSpec((bm, columns), lambda i, s: (i, 0))
    of_w = pl.BlockSpec((None, bm, columns), lambda i, s: (layer, i + s[0] * steps, 0))
    of_m = pl.BlockSpec((None, bm, columns), lambda i, s: (layer, i, 0))
    aliased = [] if so_far is None else list(so_far)
    return pl.pallas_call(
        body,
        grid_spec=pltpu.PrefetchScalarGridSpec(
            num_scalar_prefetch=1,
            grid=(steps,),
            in_specs=specs + [of_w, of_m, of_m] + [pl.BlockSpec(memory_space=pl.ANY)] * len(aliased),
            out_specs=[plain, of_w, of_m, of_m],
        ),
        out_shape=[
            jax.ShapeDtypeStruct((rows, columns), BF16),
            jax.ShapeDtypeStruct(w.shape, BF16),
            jax.ShapeDtypeStruct(m.shape, F32),
            jax.ShapeDtypeStruct(v.shape, F32),
        ],
        input_output_aliases={1 + count + 3 + i: 1 + i for i in range(len(aliased))},
        compiler_params=params(1),
        cost_estimate=pl.CostEstimate(flops=10**9, bytes_accessed=rows * columns * 28, transcendentals=0),
        name="adamw",
    )(place, *arrays, w, m, v, *aliased)


def place(new, blocks, positions, layer, steps=3):
    rows, columns = blocks[0].shape
    bm = rows // steps
    count = len(blocks)

    def body(at, *refs):
        for which in range(count):

            @pl.when(pl.program_id(0) == which)
            def _():
                refs[-1][...] = refs[which][...]

    def of_block(which):
        return pl.BlockSpec((bm, columns), lambda k, i, at: (jnp.where(k == which, i, jnp.where(k < which, 0, steps - 1)), 0))

    return pl.pallas_call(
        body,
        grid_spec=pltpu.PrefetchScalarGridSpec(
            num_scalar_prefetch=1,
            grid=(count, steps),
            in_specs=[of_block(which) for which in range(count)] + [pl.BlockSpec(memory_space=pl.ANY)],
            out_specs=pl.BlockSpec((None, bm, columns), lambda k, i, at: (layer, at[k] * steps + i, 0)),
        ),
        out_shape=jax.ShapeDtypeStruct(new.shape, new.dtype),
        input_output_aliases={count + 1: 0},
        compiler_params=params(2),
        cost_estimate=pl.CostEstimate(flops=10**9, bytes_accessed=4 * count * rows * columns, transcendentals=0),
        name="place",
    )(jnp.stack(positions), *blocks, new)


def step(x, dy, w_gate, w_up, w_down, *moments):
    x, dy = x[0], dy[0]
    index = lax.axis_index("dp").astype(jnp.int32)
    chip, core = index // 2, index % 2

    def across(t):
        return lax.ppermute(t, "dp", CROSS)

    def within(t):
        return lax.ppermute(t, "dp", INCHIP)

    dy_far = across(dy)
    a0, gate0, up0, act0 = gates(x, w_gate, w_up, 0)
    h1 = down(act0, w_down, x, 0)
    f = act0.shape[1]
    kept = f - f // 2 // BN * BN
    h1_far = across(h1)
    a1, act1, d_gate1, d_up1 = last_layer(h1, dy, w_gate, w_up, w_down, 1, chip, kept)
    dh1 = into_layer(d_gate1, d_up1, w_gate, w_up, h1, dy, 1)

    def group_sum(g, whole=True):
        rows = g.shape[0] // 4
        blocks = g.reshape(4, rows, g.shape[1])
        far_block = (1 - chip) * 2 + core
        if whole:
            near = within(g)
            theirs = lax.dynamic_index_in_dim(near.reshape(blocks.shape), far_block, 0, False)
        else:
            near = within(lax.dynamic_index_in_dim(g.reshape(2, 2, rows, g.shape[1]), 1 - core, 1, keepdims=False))
            theirs = lax.dynamic_index_in_dim(near, 1 - chip, 0, False)
        ours = lax.dynamic_index_in_dim(blocks, far_block, 0, False)
        far = across((ours.astype(F32) + theirs.astype(F32)).astype(BF16))
        return [(g, 0), (near, 0 if whole else 1), (far, None)]

    _, d = x.shape
    terms0 = {name: [] for name in "gud"}
    for number, name in enumerate("abc"):
        g = weight_gradient([(act0, dh1)], 1408, d // 3, piece=number)
        terms0["d"].append(group_sum(g, name != "c"))
    cut = 6 * BN
    for name, first, columns, bn in (("a", 0, cut, 512), ("b", cut, f - cut, BN)):
        d_gate0, d_up0 = to_gates(dh1, w_down, gate0, up0, 0, first, columns)
        g = weight_gradient([(a0, d_gate0)], d, bn)
        terms0["g"].append(group_sum(g, name != "a"))
        g = weight_gradient([(a0, d_up0)], d, bn)
        terms0["u"].append(group_sum(g))

    h1_far, _ = lax.optimization_barrier((h1_far, g))
    a1_far, act1_far, d_gate1_far, d_up1_far = last_layer(h1_far, dy_far, w_gate, w_up, w_down, 1, chip, kept)
    g_down1 = weight_gradient([(act1, dy), (act1_far, dy_far)], kept, 512, None, kept)
    half = d // 2
    g_gate1 = weight_gradient([(a1, d_gate1), (a1_far, d_gate1_far)], half, 512, chip, half)
    g_up1 = weight_gradient([(a1, d_up1), (a1_far, d_up1_far)], half, 512, chip, half)

    def of_the_chip(g, rows, offset=None):
        start = 0 if offset is None else offset
        near = within(lax.dynamic_slice_in_dim(g, start + (1 - core) * rows, rows, 0))
        ours = (g, 2) if offset is None else (lax.dynamic_slice_in_dim(g, start + core * rows, rows, 0), None)
        return [[ours, (near, None)]]

    terms1 = {
        "g": of_the_chip(g_gate1, half // 2),
        "u": of_the_chip(g_up1, half // 2),
        "d": of_the_chip(g_down1, f // 4, chip * (f // 2 - (f - kept))),
    }

    here = jnp.stack([index, chip, core])
    at_near, at_far, at_newer = chip * 2 + 1 - core, (1 - chip) * 2 + core, (1 - chip) * 2 + 1 - core
    new = []
    for which, name in enumerate("gud"):
        w, m, v = (w_gate, w_up, w_down)[which], moments[which], moments[3 + which]
        own0, *so_far = adamw(terms0[name], w, m, v, 0, here, None)
        own1, w_new, m_new, v_new = adamw(terms1[name], w, m, v, 1, here, so_far)
        for layer, own in ((0, own0), (1, own1)):
            label = name + str(layer)
            near = within(own)
            if label != "d1":
                far = across(own)
                newer = within(far)
                w_new = place(w_new, (near, far, newer), (at_near, at_far, at_newer), layer)
                continue
            rows = own.shape[0] // 2
            far = [across(own[part * rows :][:rows]) for part in (0, 1)]
            newer = [within(t) for t in far]
            w_new = place(w_new, (near,), (at_near,), layer)
            w_new = place(w_new, (far[0], newer[0]), (at_far * 2, at_newer * 2), layer)
            w_new = place(w_new, (far[1],), (at_far * 2 + 1,), layer)
            w_new = place(w_new, (newer[1],), (at_newer * 2 + 1,), layer)
        new.append((w_new, m_new, v_new))
    return tuple(one[which] for which in range(3) for one in new)


def solution(mesh):
    sequences, whole, rows, group = P(("rep", "dp")), P(), P(None, "dp"), P("rep")

    return jax.shard_map(
        step,
        mesh=mesh,
        in_specs=(sequences,) * 2 + (whole,) * 3 + (rows,) * 6,
        out_specs=(group,) * 3 + (P("rep", "dp"),) * 6,
        check_vma=False,
    )
```
